32 devices in a mesh: zero: 2 (over core), cols: 4 (over y, x), ens: 4 (over z).
Axes of the slice: x: 2, y: 2, z: 4, core: 2. Of those that a mesh axis runs over, the one named last changes fastest.
Arguments:
- weight_gate: float32 [8192, 8192], P(('ens', 'zero'), 'cols'), parts along dimension 0, may hold values from -0.1875 to 0.1875
- moment_gate: float32 [8192, 8192], P(('ens', 'zero'), 'cols'), parts along dimension 0, may hold values from -0.125 to 0.125
- square_gate: float32 [8192, 8192], P(('ens', 'zero'), 'cols'), parts along dimension 0, may hold values from -0.125 to 0.125
- weight_up: float32 [8192, 8192], P(('ens', 'zero'), 'cols'), parts along dimension 0, may hold values from -0.1875 to 0.1875
- moment_up: float32 [8192, 8192], P(('ens', 'zero'), 'cols'), parts along dimension 0, may hold values from -0.125 to 0.125
- square_up: float32 [8192, 8192], P(('ens', 'zero'), 'cols'), parts along dimension 0, may hold values from -0.125 to 0.125
- norm_gain: float32 [8192], P(('ens', 'zero')), parts along dimension 0, may hold values from 0.25 to 1.75
Outputs:
- ready_gate: bfloat16 [8192, 8192], P('ens', 'cols'), parts along dimension 0
- ready_up: bfloat16 [8192, 8192], P('ens', 'cols'), parts along dimension 0
- factor_gate: float32 [32768], P(('ens', 'cols')), parts along dimension 0
- factor_up: float32 [32768], P(('ens', 'cols')), parts along dimension 0
The draws below stay inside these ranges and needn't reach their ends.
There are 4 independent parts, one for each index of `ens`. The reference program is written for one: setup_inputs(seed, part) draws one part's arguments, and reference() takes and returns one part's arrays. A program takes and returns all parts, laid end to end along the dimension named above; each array names one. Nothing has to cross between parts.
All inputs are finite; a program needn't handle non-finite values. Where the reference program divides by a largest or mean magnitude, that divisor is 1e-20 or more.
Results may differ from the reference program's by a relative error of at most 0.001.
Values may be sent and summed in bfloat16 or wider, within the bound.
A program may use at most 128 MiB of HBM per device.

```python
import jax
import jax.numpy as jnp

D_MODEL = 2048
D_INNER = 8192


def raised(array, rng, source, target, parts, factor):
    owner, partner = [(jnp.arange(array.shape[axis_at]) // (array.shape[axis_at] // parts)).reshape([-1 if axis == axis_at else 1 for axis in range(array.ndim)]) for axis_at in (source, target)]
    chosen = jax.random.permutation(rng, parts)[partner]
    strong = (owner == chosen) | (owner == (partner + parts // 2) % parts)
    return jnp.where(strong, factor * array, array)


def steps_of(stream_key, extent, shards, smallest, high):
    loudness = 1.0
    for axis_at, shards_of in shards:
        heights = jax.random.uniform(jax.random.fold_in(jax.random.fold_in(stream_key, 6), axis_at), (shards_of,), jnp.float32, smallest / len(shards), high / len(shards))
        loudness = loudness * jnp.repeat(jnp.exp(heights), extent[axis_at] // shards_of).reshape((-1,) + (1,) * (len(extent) - 1 - axis_at))
    return loudness


def noise(rng, extent, spread, reach, cuts=(), kind=jnp.bfloat16):
    loudness = steps_of(rng, extent, cuts, -0.22, 0.18) if cuts else 1.0
    values = jax.random.normal(rng, extent, jnp.float32) * spread * loudness
    return jnp.minimum(jnp.maximum(values, -reach), reach).astype(kind)


def heavy_noise(own_key, extent, width, most, cuts, heavy, held_as=jnp.bfloat16):
    array = width * jax.random.normal(own_key, extent, jnp.float32)
    if cuts:
        array = array * steps_of(own_key, extent, cuts, -0.22, 0.18)
    return jnp.clip(raised(array, jax.random.fold_in(own_key, 3), *heavy), -most, most).astype(held_as)


def setup_inputs(seed: int = 0, part: int = 0) -> dict:
    keys = jax.random.split(jax.random.key(seed), 8)
    own_keys = jax.random.split(jax.random.fold_in(keys[7], part), 8)
    weight_gate = heavy_noise(own_keys[0], (D_MODEL, D_INNER), D_MODEL ** -0.5, 0.1875, ((0, 2), (1, 4)), (0, 1, 4, 2.0), jnp.float32)
    moment_gate = noise(own_keys[1], (D_MODEL, D_INNER), D_MODEL ** -0.5, 0.125, ((0, 2), (1, 4)), jnp.float32)
    square_gate = noise(own_keys[2], (D_MODEL, D_INNER), D_MODEL ** -0.5, 0.125, ((0, 2), (1, 4)), jnp.float32)
    weight_up = heavy_noise(own_keys[3], (D_MODEL, D_INNER), D_MODEL ** -0.5, 0.1875, ((0, 2), (1, 4)), (0, 1, 4, 2.0), jnp.float32)
    moment_up = noise(own_keys[4], (D_MODEL, D_INNER), D_MODEL ** -0.5, 0.125, ((0, 2), (1, 4)), jnp.float32)
    square_up = noise(own_keys[5], (D_MODEL, D_INNER), D_MODEL ** -0.5, 0.125, ((0, 2), (1, 4)), jnp.float32)
    norm_gain = jnp.clip(1.0 + 0.15 * jax.random.normal(own_keys[6], (D_MODEL,), jnp.float32), 0.25, 1.75)
    return {"weight_gate": weight_gate, "moment_gate": moment_gate, "square_gate": square_gate, "weight_up": weight_up, "moment_up": moment_up, "square_up": square_up, "norm_gain": norm_gain}


learn_rate = 0.2
hold_rate = 0.9


def reference(weight_gate, moment_gate, square_gate, weight_up, moment_up, square_up, norm_gain):
    hold_gate = hold_rate * moment_gate + square_gate
    latest_gate = weight_gate - learn_rate * hold_gate
    hold_up = hold_rate * moment_up + square_up
    latest_up = weight_up - learn_rate * hold_up
    latest_gained_gate = latest_gate * norm_gain[:, None]
    latest_gained_up = latest_up * norm_gain[:, None]
    factor_gate = jnp.max(jnp.abs(latest_gained_gate), axis=0)
    ready_gate = (latest_gained_gate / factor_gate).astype(jnp.bfloat16)
    factor_up = jnp.max(jnp.abs(latest_gained_up), axis=0)
    ready_up = (latest_gained_up / factor_up).astype(jnp.bfloat16)
    return ready_gate, ready_up, factor_gate, factor_up
```

```python
import functools

import jax
import jax.numpy as jnp
from jax import lax
from jax.experimental import pallas as pl
from jax.experimental.pallas import tpu as pltpu
from jax.sharding import PartitionSpec as P

MESH = pl.DeviceIdType.MESH
learn_rate = 0.2
hold_rate = 0.9
LANES = 128
SLOTS = 10
LAG_COLUMNS = 256
BUDGET = 1024
WIDE = 256
PIECES = 4


def kernel(
    n, plan, block,
    weight_gate, moment_gate, square_gate, weight_up, moment_up, square_up, gain_ref,
    ready_gate, ready_up, factor_gate, factor_up,
    held, gain_near, gain_wide, peaks, gain_sem, load_sem, peak_send, peak_recv, out_send, out_recv,
):
    rows, columns = weight_gate.shape
    steps = len(plan)
    me = lax.axis_index("zero")
    partners = [lax.rem(me + k, n) for k in range(1, n)]
    sources = ((weight_gate, moment_gate, square_gate), (weight_up, moment_up, square_up))
    readies = (ready_gate, ready_up)
    factors = (factor_gate, factor_up)

    def place(step):
        which, start, width = plan[step]
        return which, pl.ds(start, width), width

    def loads(step):
        which, span, width = place(step)
        slot = step % SLOTS
        return [
            pltpu.make_async_copy(source.at[:, span], held.at[slot, k, :, pl.ds(0, width)], load_sem.at[slot, k])
            for k, source in enumerate(sources[which])
        ]

    def swaps(step):
        width = plan[step][2]
        return [
            pltpu.make_async_remote_copy(
                src_ref=peaks.at[step, 0, :, pl.ds(0, width)],
                dst_ref=peaks.at[step, k + 1, :, pl.ds(0, width)],
                send_sem=peak_send.at[step, k],
                recv_sem=peak_recv.at[step, k],
                device_id={"zero": partner},
                device_id_type=MESH,
            )
            for k, partner in enumerate(partners)
        ]

    def sends(step):
        which, span, width = place(step)
        mine = readies[which].at[pl.ds(pl.multiple_of(me * rows, rows), rows), span]
        return [
            pltpu.make_async_remote_copy(
                src_ref=mine,
                dst_ref=mine,
                send_sem=out_send.at[step, k],
                recv_sem=out_recv.at[step, k],
                device_id={"zero": partner},
                device_id_type=MESH,
            )
            for k, partner in enumerate(partners)
        ]

    def update(step):
        slot = step % SLOTS

        def body(i, tops):
            span = pl.ds(pl.multiple_of(i * block, block), block)
            gain = gain_wide[span, :]
            new = []
            for j, top in enumerate(tops):
                lanes = pl.ds(j * LANES, LANES)
                hold = hold_rate * held[slot, 1, span, lanes] + held[slot, 2, span, lanes]
                gained = (held[slot, 0, span, lanes] - learn_rate * hold) * gain
                held[slot, 0, span, lanes] = gained
                high = jnp.max(jnp.abs(gained).reshape(block // 8, 8, LANES), axis=0)
                new.append(jnp.maximum(top, high))
            return tuple(new)

        zero = jnp.zeros((8, LANES), jnp.float32)
        tops = lax.fori_loop(0, rows // block, body, (zero,) * (plan[step][2] // LANES))
        for j, top in enumerate(tops):
            peaks[step, 0, :, pl.ds(j * LANES, LANES)] = top

    def finish(step):
        which, span, width = place(step)
        slot = step % SLOTS
        top = peaks[step, 0, :, pl.ds(0, width)]
        for k in range(1, n):
            top = jnp.maximum(top, peaks[step, k, :, pl.ds(0, width)])
        factor = jnp.max(top, axis=0, keepdims=True)
        factors[which][:, span] = factor
        scale = jnp.broadcast_to(1.0 / factor, (block, width))
        ready = readies[which]

        def body(i, carry):
            span_in = pl.ds(pl.multiple_of(i * block, block), block)
            span_out = pl.ds(pl.multiple_of(me * rows + i * block, block), block)
            ready[span_out, span] = (held[slot, 0, span_in, pl.ds(0, width)] * scale).astype(ready.dtype)
            return carry

        lax.fori_loop(0, rows // block, body, 0)

    gain_copy = pltpu.make_async_copy(gain_ref, gain_near, gain_sem)
    gain_copy.start()
    issued = 0

    def feed(waited, finished):
        nonlocal issued
        while issued < steps and issued < finished + SLOTS:
            ahead = sum(width for _, _, width in plan[waited:issued + 1])
            if ahead > BUDGET:
                break
            for copy in loads(issued):
                copy.start(priority=1)
            issued += 1

    feed(0, 0)

    barrier = pltpu.get_barrier_semaphore()
    for partner in partners:
        pl.semaphore_signal(barrier, inc=1, device_id={"zero": partner}, device_id_type=MESH)

    gain_copy.wait()
    for k in range(rows // LANES):
        wide = jnp.broadcast_to(gain_near[k:k + 1, :], (LANES, LANES))
        gain_wide[pl.ds(k * LANES, LANES), :] = wide.T

    pl.semaphore_wait(barrier, n - 1)

    done = 0
    for step in range(steps):
        for copy in loads(step):
            copy.wait()
        feed(step + 1, done)
        update(step)
        for copy in swaps(step):
            copy.start()
        while done <= step and (step + 1 == steps or sum(width for _, _, width in plan[done + 1:step + 1]) >= LAG_COLUMNS):
            for copy in swaps(done):
                copy.wait_recv()
            finish(done)
            for copy in sends(done):
                copy.start()
            done += 1
            feed(step + 1, done)

    for step in range(steps):
        for copy in swaps(step):
            copy.wait_send()
        for copy in sends(step):
            copy.wait()


def write_out(*refs):
    nears, fars, sem = refs[:4], refs[4:8], refs[8]
    copies = []
    for near, far in zip(nears[:2], fars[:2]):
        rows = near.shape[0] // PIECES
        for k in range(PIECES):
            span = pl.ds(k * rows, rows)
            copies.append((near.at[span], far.at[span]))
    copies += list(zip(nears[2:], fars[2:]))
    copies = [pltpu.make_async_copy(*pair, sem.at[k]) for k, pair in enumerate(copies)]
    for copy in copies:
        copy.start()
    for copy in copies:
        copy.wait()


def cut(columns):
    plan = []
    for which in range(2):
        for start in range(0, columns, WIDE):
            plan.append((which, start, min(WIDE, columns - start)))
    return tuple(plan)


def solution(mesh):
    n = mesh.shape["zero"]

    def per_device(weight_gate, moment_gate, square_gate, weight_up, moment_up, square_up, norm_gain):
        rows, columns = weight_gate.shape
        plan = cut(columns)
        chunk = max(width for _, _, width in plan)
        block = 64
        steps = len(plan)
        ready = pltpu.VMEM((n * rows, columns), jnp.bfloat16)
        factor = pltpu.VMEM((1, columns), jnp.float32)
        hbm = pl.BlockSpec(memory_space=pltpu.HBM)
        vmem = pl.BlockSpec(memory_space=pltpu.VMEM)
        ready_gate, ready_up, factor_gate, factor_up = pl.pallas_call(
            functools.partial(kernel, n, plan, block),
            out_shape=(ready, ready, factor, factor),
            in_specs=[hbm] * 7,
            out_specs=(vmem,) * 4,
            scratch_shapes=[
                pltpu.VMEM((SLOTS, 3, rows, chunk), jnp.float32),
                pltpu.VMEM((rows // LANES, LANES), jnp.float32),
                pltpu.VMEM((rows, LANES), jnp.float32),
                pltpu.VMEM((steps, n, 8, chunk), jnp.float32),
                pltpu.SemaphoreType.DMA,
                pltpu.SemaphoreType.DMA((SLOTS, 3)),
                pltpu.SemaphoreType.DMA((steps, n - 1)),
                pltpu.SemaphoreType.DMA((steps, n - 1)),
                pltpu.SemaphoreType.DMA((steps, n - 1)),
                pltpu.SemaphoreType.DMA((steps, n - 1)),
            ],
            compiler_params=pltpu.CompilerParams(
                collective_id=0, has_side_effects=True, vmem_limit_bytes=46 * 2 ** 20
            ),
        )(
            weight_gate, moment_gate, square_gate, weight_up, moment_up, square_up,
            norm_gain.reshape(rows // LANES, LANES),
        )
        near = (ready_gate, ready_up, factor_gate.reshape(columns), factor_up.reshape(columns))
        return pl.pallas_call(
            write_out,
            out_shape=tuple(jax.ShapeDtypeStruct(part.shape, part.dtype) for part in near),
            in_specs=[vmem] * 4,
            out_specs=(hbm,) * 4,
            scratch_shapes=[pltpu.SemaphoreType.DMA((2 * PIECES + 2,))],
            compiler_params=pltpu.CompilerParams(vmem_limit_bytes=2 ** 20),
        )(*near)

    split = P(("ens", "zero"), "cols")
    return jax.shard_map(
        per_device,
        mesh=mesh,
        in_specs=(split,) * 6 + (P(("ens", "zero")),),
        out_specs=(P("ens", "cols"), P("ens", "cols"), P(("ens", "cols")), P(("ens", "cols"))),
        check_vma=False,
    )
```

```python
import functools

import jax
import jax.numpy as jnp
from jax import lax
from jax.experimental import pallas as pl
from jax.experimental.pallas import tpu as pltpu
from jax.sharding import PartitionSpec as P

MESH = pl.DeviceIdType.MESH
learn_rate = 0.2
hold_rate = 0.9
LANES = 128
SLOTS = 7
AHEAD = 4
LAG = 1
RING = 4
WIDE = 256
PIECES = 4


def kernel(
    n, plan, block,
    weight_gate, moment_gate, square_gate, weight_up, moment_up, square_up, gain_ref,
    ready_gate, ready_up, factor_gate, factor_up,
    held, gain_near, gain_wide, peaks, gain_sem, load_sem, peak_send, peak_recv, out_send, out_recv,
):
    rows, columns = weight_gate.shape
    steps = len(plan)
    width = held.shape[-1]
    me = lax.axis_index("zero")
    partners = [lax.rem(me + k, n) for k in range(1, n)]
    sources = ((weight_gate, moment_gate, square_gate), (weight_up, moment_up, square_up))
    readies = (ready_gate, ready_up)
    factors = (factor_gate, factor_up)

    def place(step):
        which, start = plan[step]
        return which, pl.ds(start, width)

    def rows_of(device):
        return pl.ds(pl.multiple_of(device * rows, rows), rows)

    def load(step):
        which, span = place(step)
        slot = step % SLOTS
        for k, source in enumerate(sources[which]):
            pltpu.make_async_copy(source.at[:, span], held.at[slot, k], load_sem.at[slot]).start(priority=1)

    def loaded(step):
        slot = step % SLOTS
        pltpu.make_async_copy(held.at[slot], held.at[slot], load_sem.at[slot]).wait()

    def to_partner(k, src, dst, send_sem, recv_sem):
        return pltpu.make_async_remote_copy(
            src_ref=src,
            dst_ref=dst,
            send_sem=send_sem,
            recv_sem=recv_sem,
            device_id={"zero": partners[k]},
            device_id_type=MESH,
        )

    def swaps(step):
        return [
            to_partner(
                k, peaks.at[0, step], peaks.at[k + 1, step], peak_send.at[k], peak_recv.at[step % RING, k]
            )
            for k in range(n - 1)
        ]

    def sends(step):
        which, span = place(step)
        mine = readies[which].at[rows_of(me), span]
        return [to_partner(k, mine, mine, out_send.at[which, k], out_recv.at[which, k]) for k in range(n - 1)]

    def update(step):
        slot = step % SLOTS

        def body(i, tops):
            span = pl.ds(pl.multiple_of(i * block, block), block)
            gain = gain_wide[span, :]
            new = []
            for j, top in enumerate(tops):
                lanes = pl.ds(j * LANES, LANES)
                hold = hold_rate * held[slot, 1, span, lanes] + held[slot, 2, span, lanes]
                gained = (held[slot, 0, span, lanes] - learn_rate * hold) * gain
                held[slot, 0, span, lanes] = gained
                high = jnp.max(jnp.abs(gained).reshape(block // 8, 8, LANES), axis=0)
                new.append(jnp.maximum(top, high))
            return tuple(new)

        zero = jnp.zeros((8, LANES), jnp.float32)
        tops = lax.fori_loop(0, rows // block, body, (zero,) * (width // LANES))
        for j, top in enumerate(tops):
            peaks[0, step, :, pl.ds(j * LANES, LANES)] = top

    def finish(step):
        which, span = place(step)
        slot = step % SLOTS
        top = peaks[0, step]
        for k in range(1, n):
            top = jnp.maximum(top, peaks[k, step])
        factor = jnp.max(top, axis=0, keepdims=True)
        factors[which][:, span] = factor
        scale = jnp.broadcast_to(1.0 / factor, (block, width))
        ready = readies[which]

        def body(i, carry):
            span_in = pl.ds(pl.multiple_of(i * block, block), block)
            span_out = pl.ds(pl.multiple_of(me * rows + i * block, block), block)
            ready[span_out, span] = (held[slot, 0, span_in, :] * scale).astype(ready.dtype)
            return carry

        lax.fori_loop(0, rows // block, body, 0)

    gain_copy = pltpu.make_async_copy(gain_ref, gain_near, gain_sem)
    gain_copy.start()
    for step in range(min(AHEAD, steps)):
        load(step)

    barrier = pltpu.get_barrier_semaphore()
    for partner in partners:
        pl.semaphore_signal(barrier, inc=1, device_id={"zero": partner}, device_id_type=MESH)

    gain_copy.wait()
    for k in range(rows // LANES):
        wide = jnp.broadcast_to(gain_near[k:k + 1, :], (LANES, LANES))
        gain_wide[pl.ds(k * LANES, LANES), :] = wide.T

    pl.semaphore_wait(barrier, n - 1)

    for step in range(steps + LAG):
        if step < steps:
            loaded(step)
            if step + AHEAD < steps:
                load(step + AHEAD)
            update(step)
            for copy in swaps(step):
                copy.start()
        done = step - LAG
        if done >= 0:
            for copy in swaps(done):
                copy.wait_recv()
            finish(done)
            for copy in sends(done):
                copy.start()

    for k, partner in enumerate(partners):
        to_partner(k, peaks.at[0], peaks.at[0], peak_send.at[k], peak_recv.at[0, k]).wait_send()
        for which, ready in enumerate(readies):
            mine = ready.at[rows_of(me)]
            copy = to_partner(k, mine, mine, out_send.at[which, k], out_recv.at[which, k])
            copy.wait()


def write_out(*refs):
    nears, fars, sem = refs[:4], refs[4:8], refs[8]
    for k, (near, far) in enumerate(zip(nears, fars)):
        pieces = PIECES if k < 2 else 1
        rows = near.shape[0] // pieces
        for piece in range(pieces):
            span = pl.ds(piece * rows, rows)
            pltpu.make_async_copy(near.at[span], far.at[span], sem.at[k]).start()
    for k, (near, far) in enumerate(zip(nears, fars)):
        pltpu.make_async_copy(near, far, sem.at[k]).wait()


def solution(mesh):
    n = mesh.shape["zero"]

    def per_device(weight_gate, moment_gate, square_gate, weight_up, moment_up, square_up, norm_gain):
        rows, columns = weight_gate.shape
        wide = WIDE if columns % WIDE == 0 else LANES
        plan = tuple((which, start) for which in range(2) for start in range(0, columns, wide))
        block = 128
        steps = len(plan)
        ready = pltpu.VMEM((n * rows, columns), jnp.bfloat16)
        factor = pltpu.VMEM((1, columns), jnp.float32)
        hbm = pl.BlockSpec(memory_space=pltpu.HBM)
        vmem = pl.BlockSpec(memory_space=pltpu.VMEM)
        ready_gate, ready_up, factor_gate, factor_up = pl.pallas_call(
            functools.partial(kernel, n, plan, block),
            out_shape=(ready, ready, factor, factor),
            in_specs=[hbm] * 7,
            out_specs=(vmem,) * 4,
            scratch_shapes=[
                pltpu.VMEM((SLOTS, 3, rows, wide), jnp.float32),
                pltpu.VMEM((rows // LANES, LANES), jnp.float32),
                pltpu.VMEM((rows, LANES), jnp.float32),
                pltpu.VMEM((n, steps, 8, wide), jnp.float32),
                pltpu.SemaphoreType.DMA,
                pltpu.SemaphoreType.DMA((SLOTS,)),
                pltpu.SemaphoreType.DMA((n - 1,)),
                pltpu.SemaphoreType.DMA((RING, n - 1)),
                pltpu.SemaphoreType.DMA((2, n - 1)),
                pltpu.SemaphoreType.DMA((2, n - 1)),
            ],
            compiler_params=pltpu.CompilerParams(
                collective_id=0, has_side_effects=True, vmem_limit_bytes=46 * 2 ** 20
            ),
        )(
            weight_gate, moment_gate, square_gate, weight_up, moment_up, square_up,
            norm_gain.reshape(rows // LANES, LANES),
        )
        near = (ready_gate, ready_up, factor_gate.reshape(columns), factor_up.reshape(columns))
        return pl.pallas_call(
            write_out,
            out_shape=tuple(jax.ShapeDtypeStruct(part.shape, part.dtype) for part in near),
            in_specs=[vmem] * 4,
            out_specs=(hbm,) * 4,
            scratch_shapes=[pltpu.SemaphoreType.DMA((4,))],
            compiler_params=pltpu.CompilerParams(vmem_limit_bytes=2 ** 20),
        )(*near)

    split = P(("ens", "zero"), "cols")
    return jax.shard_map(
        per_device,
        mesh=mesh,
        in_specs=(split,) * 6 + (P(("ens", "zero")),),
        out_specs=(P("ens", "cols"), P("ens", "cols"), P(("ens", "cols")), P(("ens", "cols"))),
        check_vma=False,
    )
```

```python
import functools

import jax
import jax.numpy as jnp
from jax import lax
from jax.experimental import pallas as pl
from jax.experimental.pallas import tpu as pltpu
from jax.sharding import PartitionSpec as P

MESH = pl.DeviceIdType.MESH
learn_rate = 0.2
hold_rate = 0.9
LANES = 128
SLOTS = 6
AHEAD = 4
RING = 5
UPDATE = 256 * 128
WIDE = 256
SPLIT = 2
PARTS = 2
TAPER = True
PIECES = 4


def kernel(
    n, plan, block,
    weight_gate, moment_gate, square_gate, weight_up, moment_up, square_up, gain_ref,
    ready_gate, ready_up, factor_gate, factor_up,
    held, gain_near, gain_wide, peaks, gain_sem, load_sem, peak_send, peak_recv, out_send, out_recv,
):
    rows, columns = weight_gate.shape
    steps = len(plan)
    wide = held.shape[-1]
    me = lax.axis_index("zero")
    partners = [lax.rem(me + k, n) for k in range(1, n)]
    sources = ((weight_gate, moment_gate, square_gate), (weight_up, moment_up, square_up))
    readies = (ready_gate, ready_up)
    factors = (factor_gate, factor_up)

    def place(step):
        which, start, width = plan[step]
        return which, pl.ds(start, width), width

    def rows_of(device):
        return pl.ds(pl.multiple_of(device * rows, rows), rows)

    def load(step):
        which, span, width = place(step)
        slot = step % SLOTS
        for part in range(SPLIT):
            some = pl.ds(part * (rows // SPLIT), rows // SPLIT)
            for k, source in enumerate(sources[which]):
                near = held.at[slot, k, some, pl.ds(0, width)]
                pltpu.make_async_copy(source.at[some, span], near, load_sem.at[slot, part]).start(priority=1)

    def loaded(step, part):
        slot = step % SLOTS
        some = pl.ds(part * (rows // SPLIT), rows // SPLIT)
        near = held.at[slot, :, some, pl.ds(0, plan[step][2])]
        pltpu.make_async_copy(near, near, load_sem.at[slot, part]).wait()

    def to_partner(k, src, dst, send_sem, recv_sem):
        return pltpu.make_async_remote_copy(
            src_ref=src,
            dst_ref=dst,
            send_sem=send_sem,
            recv_sem=recv_sem,
            device_id={"zero": partners[k]},
            device_id_type=MESH,
        )

    def swaps(step):
        lanes = pl.ds(0, plan[step][2])
        mine = peaks.at[0, step, :, lanes]
        return [
            to_partner(k, mine, peaks.at[k + 1, step, :, lanes], peak_send.at[k], peak_recv.at[step % RING, k])
            for k in range(n - 1)
        ]

    def send(step, part):
        which, span, _ = place(step)
        some = rows // PARTS
        mine = readies[which].at[pl.ds(pl.multiple_of(me * rows + part * some, some), some), span]
        for k in range(n - 1):
            to_partner(k, mine, mine, out_send.at[which, k], out_recv.at[which, k]).start()

    def update(step, part, tops):
        slot = step % SLOTS
        block = min(UPDATE // plan[step][2], rows // SPLIT)
        first = part * (rows // SPLIT)

        def body(i, tops):
            span = pl.ds(pl.multiple_of(first + i * block, block), block)
            gain = gain_wide[span, :]
            new = []
            for j, top in enumerate(tops):
                lanes = pl.ds(j * LANES, LANES)
                hold = hold_rate * held[slot, 1, span, lanes] + held[slot, 2, span, lanes]
                gained = (held[slot, 0, span, lanes] - learn_rate * hold) * gain
                held[slot, 0, span, lanes] = gained
                high = jnp.max(jnp.abs(gained).reshape(block // 8, 8, LANES), axis=0)
                new.append(jnp.maximum(top, high))
            return tuple(new)

        return lax.fori_loop(0, rows // SPLIT // block, body, tops)

    def finish(step):
        which, span, width = place(step)
        slot = step % SLOTS
        lanes = pl.ds(0, width)
        top = peaks[0, step, :, lanes]
        for k in range(1, n):
            top = jnp.maximum(top, peaks[k, step, :, lanes])
        factor = jnp.max(top, axis=0, keepdims=True)
        factors[which][:, span] = factor
        scale = jnp.broadcast_to(1.0 / factor, (block, width))
        ready = readies[which]

        def body(i, carry):
            span_in = pl.ds(pl.multiple_of(i * block, block), block)
            span_out = pl.ds(pl.multiple_of(me * rows + i * block, block), block)
            ready[span_out, span] = (held[slot, 0, span_in, lanes] * scale).astype(ready.dtype)
            return carry

        count = rows // PARTS // block
        for part in range(PARTS):
            lax.fori_loop(part * count, (part + 1) * count, body, 0)
            send(step, part)

    gain_copy = pltpu.make_async_copy(gain_ref, gain_near, gain_sem)
    gain_copy.start()
    for step in range(min(AHEAD, steps)):
        load(step)

    barrier = pltpu.get_barrier_semaphore()
    for partner in partners:
        pl.semaphore_signal(barrier, inc=1, device_id={"zero": partner}, device_id_type=MESH)

    gain_copy.wait()
    for k in range(rows // LANES):
        gains = jnp.broadcast_to(gain_near[k:k + 1, :], (LANES, LANES))
        gain_wide[pl.ds(k * LANES, LANES), :] = gains.T

    pl.semaphore_wait(barrier, n - 1)

    done = 0
    for step in range(steps):
        tops = (jnp.zeros((8, LANES), jnp.float32),) * (plan[step][2] // LANES)
        for part in range(SPLIT):
            loaded(step, part)
            if part + 1 == SPLIT and step + AHEAD < steps:
                load(step + AHEAD)
            tops = update(step, part, tops)
        for j, top in enumerate(tops):
            peaks[0, step, :, pl.ds(j * LANES, LANES)] = top
        for copy in swaps(step):
            copy.start()
        while done < steps and (step + 1 == steps or (done < step and plan[step][2] == wide)):
            for copy in swaps(done):
                copy.wait_recv()
            finish(done)
            done += 1

    for k, partner in enumerate(partners):
        mine = peaks.at[0, pl.ds(0, 2 * columns // wide)]
        to_partner(k, mine, mine, peak_send.at[k], peak_recv.at[0, k]).wait_send()
        for which, ready in enumerate(readies):
            mine = ready.at[rows_of(me)]
            copy = to_partner(k, mine, mine, out_send.at[which, k], out_recv.at[which, k])
            copy.wait()


def write_out(*refs):
    nears, fars, sem = refs[:4], refs[4:8], refs[8]
    for k, (near, far) in enumerate(zip(nears, fars)):
        pieces = PIECES if k < 2 else 1
        rows = near.shape[0] // pieces
        for piece in range(pieces):
            span = pl.ds(piece * rows, rows)
            pltpu.make_async_copy(near.at[span], far.at[span], sem.at[k]).start()
    for k, (near, far) in enumerate(zip(nears, fars)):
        pltpu.make_async_copy(near, far, sem.at[k]).wait()


def solution(mesh):
    n = mesh.shape["zero"]

    def per_device(weight_gate, moment_gate, square_gate, weight_up, moment_up, square_up, norm_gain):
        rows, columns = weight_gate.shape
        wide = WIDE if columns % WIDE == 0 else LANES
        plan = [(which, start, wide) for which in range(2) for start in range(0, columns, wide)]
        if TAPER and wide > LANES:
            which, start, _ = plan.pop()
            plan += [(which, start + k, LANES) for k in range(0, wide, LANES)]
        block = min(128, rows // PARTS)
        steps = len(plan)
        ready = pltpu.VMEM((n * rows, columns), jnp.bfloat16)
        factor = pltpu.VMEM((1, columns), jnp.float32)
        hbm = pl.BlockSpec(memory_space=pltpu.HBM)
        vmem = pl.BlockSpec(memory_space=pltpu.VMEM)
        ready_gate, ready_up, factor_gate, factor_up = pl.pallas_call(
            functools.partial(kernel, n, plan, block),
            out_shape=(ready, ready, factor, factor),
            in_specs=[hbm] * 7,
            out_specs=(vmem,) * 4,
            scratch_shapes=[
                pltpu.VMEM((SLOTS, 3, rows, wide), jnp.float32),
                pltpu.VMEM((rows // LANES, LANES), jnp.float32),
                pltpu.VMEM((rows, LANES), jnp.float32),
                pltpu.VMEM((n, steps, 8, wide), jnp.float32),
                pltpu.SemaphoreType.DMA,
                pltpu.SemaphoreType.DMA((SLOTS, SPLIT)),
                pltpu.SemaphoreType.DMA((n - 1,)),
                pltpu.SemaphoreType.DMA((RING, n - 1)),
                pltpu.SemaphoreType.DMA((2, n - 1)),
                pltpu.SemaphoreType.DMA((2, n - 1)),
            ],
            compiler_params=pltpu.CompilerParams(
                collective_id=0, has_side_effects=True, vmem_limit_bytes=46 * 2 ** 20
            ),
        )(
            weight_gate, moment_gate, square_gate, weight_up, moment_up, square_up,
            norm_gain.reshape(rows // LANES, LANES),
        )
        near = (ready_gate, ready_up, factor_gate.reshape(columns), factor_up.reshape(columns))
        return pl.pallas_call(
            write_out,
            out_shape=tuple(jax.ShapeDtypeStruct(part.shape, part.dtype) for part in near),
            in_specs=[vmem] * 4,
            out_specs=(hbm,) * 4,
            scratch_shapes=[pltpu.SemaphoreType.DMA((4,))],
            compiler_params=pltpu.CompilerParams(vmem_limit_bytes=2 ** 20),
        )(*near)

    split = P(("ens", "zero"), "cols")
    return jax.shard_map(
        per_device,
        mesh=mesh,
        in_specs=(split,) * 6 + (P(("ens", "zero")),),
        out_specs=(P("ens", "cols"), P("ens", "cols"), P(("ens", "cols")), P(("ens", "cols"))),
        check_vma=False,
    )
```

```python
import functools

import jax
import jax.numpy as jnp
from jax import lax
from jax.experimental import pallas as pl
from jax.experimental.pallas import tpu as pltpu
from jax.sharding import PartitionSpec as P

MESH = pl.DeviceIdType.MESH
learn_rate = 0.2
hold_rate = 0.9
LANES = 128
SLOTS = 5
AHEAD = 3
RING = 5
UPDATE = 256 * 128
WIDE = 256
SPLIT = 2
PARTS = 2
TAPER = True
PIECES = 4


def kernel(
    n, plan, block,
    weight_gate, moment_gate, square_gate, weight_up, moment_up, square_up, gain_ref,
    ready_gate, ready_up, factor_gate, factor_up,
    held, gain_near, gain_wide, peaks, gain_sem, load_sem, peak_send, peak_recv, out_send, out_recv,
):
    rows, columns = weight_gate.shape
    steps = len(plan)
    wide = held.shape[-1]
    me = lax.axis_index("zero")
    partners = [lax.rem(me + k, n) for k in range(1, n)]
    sources = ((weight_gate, moment_gate, square_gate), (weight_up, moment_up, square_up))
    readies = (ready_gate, ready_up)
    factors = (factor_gate, factor_up)

    def place(step):
        which, start, width = plan[step]
        return which, pl.ds(start, width), width

    def rows_of(device):
        return pl.ds(pl.multiple_of(device * rows, rows), rows)

    def load(step):
        which, span, width = place(step)
        slot = step % SLOTS
        for part in range(SPLIT):
            some = pl.ds(part * (rows // SPLIT), rows // SPLIT)
            for k, source in enumerate(sources[which]):
                near = held.at[slot, k, some, pl.ds(0, width)]
                pltpu.make_async_copy(source.at[some, span], near, load_sem.at[slot, part]).start(priority=1)

    def loaded(step, part):
        slot = step % SLOTS
        some = pl.ds(part * (rows // SPLIT), rows // SPLIT)
        near = held.at[slot, :, some, pl.ds(0, plan[step][2])]
        pltpu.make_async_copy(near, near, load_sem.at[slot, part]).wait()

    def to_partner(k, src, dst, send_sem, recv_sem):
        return pltpu.make_async_remote_copy(
            src_ref=src,
            dst_ref=dst,
            send_sem=send_sem,
            recv_sem=recv_sem,
            device_id={"zero": partners[k]},
            device_id_type=MESH,
        )

    def swaps(step):
        lanes = pl.ds(0, plan[step][2])
        mine = peaks.at[0, step, :, lanes]
        return [
            to_partner(k, mine, peaks.at[k + 1, step, :, lanes], peak_send.at[k], peak_recv.at[step % RING, k])
            for k in range(n - 1)
        ]

    def send(step, part):
        which, span, _ = place(step)
        some = rows // PARTS
        mine = readies[which].at[pl.ds(pl.multiple_of(me * rows + part * some, some), some), span]
        for k in range(n - 1):
            to_partner(k, mine, mine, out_send.at[which, k], out_recv.at[which, k]).start()

    def update(step, part, tops):
        slot = step % SLOTS
        block = min(UPDATE // plan[step][2], rows // SPLIT)
        first = part * (rows // SPLIT)

        def body(i, tops):
            span = pl.ds(pl.multiple_of(first + i * block, block), block)
            gain = gain_wide[span, :]
            new = []
            for j, top in enumerate(tops):
                lanes = pl.ds(j * LANES, LANES)
                hold = hold_rate * held[slot, 1, span, lanes] + held[slot, 2, span, lanes]
                gained = (held[slot, 0, span, lanes] - learn_rate * hold) * gain
                held[slot, 0, span, lanes] = gained
                high = jnp.max(jnp.abs(gained).reshape(block // 8, 8, LANES), axis=0)
                new.append(jnp.maximum(top, high))
            return tuple(new)

        return lax.fori_loop(0, rows // SPLIT // block, body, tops)

    def finish(step):
        which, span, width = place(step)
        slot = step % SLOTS
        lanes = pl.ds(0, width)
        top = peaks[0, step, :, lanes]
        for k in range(1, n):
            top = jnp.maximum(top, peaks[k, step, :, lanes])
        factor = jnp.max(top, axis=0, keepdims=True)
        factors[which][:, span] = factor
        scale = jnp.broadcast_to(1.0 / factor, (block, width))
        ready = readies[which]

        def body(i, carry):
            span_in = pl.ds(pl.multiple_of(i * block, block), block)
            span_out = pl.ds(pl.multiple_of(me * rows + i * block, block), block)
            ready[span_out, span] = (held[slot, 0, span_in, lanes] * scale).astype(ready.dtype)
            return carry

        count = rows // PARTS // block
        for part in range(PARTS):
            lax.fori_loop(part * count, (part + 1) * count, body, 0)
            send(step, part)

    gain_copy = pltpu.make_async_copy(gain_ref, gain_near, gain_sem)
    gain_copy.start()
    for step in range(min(AHEAD, steps)):
        load(step)

    barrier = pltpu.get_barrier_semaphore()
    for partner in partners:
        pl.semaphore_signal(barrier, inc=1, device_id={"zero": partner}, device_id_type=MESH)

    gain_copy.wait()
    for k in range(rows // LANES):
        gains = jnp.broadcast_to(gain_near[k:k + 1, :], (LANES, LANES))
        gain_wide[pl.ds(k * LANES, LANES), :] = gains.T

    pl.semaphore_wait(barrier, n - 1)

    done = 0
    for step in range(steps):
        tops = (jnp.zeros((8, LANES), jnp.float32),) * (plan[step][2] // LANES)
        for part in range(SPLIT):
            loaded(step, part)
            if part + 1 == SPLIT and step + AHEAD < steps:
                load(step + AHEAD)
            tops = update(step, part, tops)
        for j, top in enumerate(tops):
            peaks[0, step, :, pl.ds(j * LANES, LANES)] = top
        for copy in swaps(step):
            copy.start()
        while done < steps and (step + 1 == steps or (done < step and plan[step][2] == wide)):
            for copy in swaps(done):
                copy.wait_recv()
            finish(done)
            done += 1

    for k, partner in enumerate(partners):
        mine = peaks.at[0, pl.ds(0, 2 * columns // wide)]
        to_partner(k, mine, mine, peak_send.at[k], peak_recv.at[0, k]).wait_send()
        for which, ready in enumerate(readies):
            mine = ready.at[rows_of(me)]
            copy = to_partner(k, mine, mine, out_send.at[which, k], out_recv.at[which, k])
            copy.wait()


def write_out(*refs):
    nears, fars, sem = refs[:4], refs[4:8], refs[8]
    pairs = list(enumerate(zip(nears, fars)))
    for k, (near, far) in pairs[2:] + pairs[:2]:
        pieces = PIECES if k < 2 else 1
        rows = near.shape[0] // pieces
        for piece in range(pieces):
            span = pl.ds(piece * rows, rows)
            pltpu.make_async_copy(near.at[span], far.at[span], sem.at[k]).start()
    for k, (near, far) in enumerate(zip(nears, fars)):
        pltpu.make_async_copy(near, far, sem.at[k]).wait()


def solution(mesh):
    n = mesh.shape["zero"]

    def per_device(weight_gate, moment_gate, square_gate, weight_up, moment_up, square_up, norm_gain):
        rows, columns = weight_gate.shape
        wide = WIDE if columns % WIDE == 0 else LANES
        plan = [(which, start, wide) for which in range(2) for start in range(0, columns, wide)]
        if TAPER and wide > LANES:
            which, start, _ = plan.pop()
            plan += [(which, start + k, LANES) for k in range(0, wide, LANES)]
        block = min(128, rows // PARTS)
        steps = len(plan)
        ready = pltpu.VMEM((n * rows, columns), jnp.bfloat16)
        factor = pltpu.VMEM((1, columns), jnp.float32)
        hbm = pl.BlockSpec(memory_space=pltpu.HBM)
        vmem = pl.BlockSpec(memory_space=pltpu.VMEM)
        ready_gate, ready_up, factor_gate, factor_up = pl.pallas_call(
            functools.partial(kernel, n, plan, block),
            out_shape=(ready, ready, factor, factor),
            in_specs=[hbm] * 7,
            out_specs=(vmem,) * 4,
            scratch_shapes=[
                pltpu.VMEM((SLOTS, 3, rows, wide), jnp.float32),
                pltpu.VMEM((rows // LANES, LANES), jnp.float32),
                pltpu.VMEM((rows, LANES), jnp.float32),
                pltpu.VMEM((n, steps, 8, wide), jnp.float32),
                pltpu.SemaphoreType.DMA,
                pltpu.SemaphoreType.DMA((SLOTS, SPLIT)),
                pltpu.SemaphoreType.DMA((n - 1,)),
                pltpu.SemaphoreType.DMA((RING, n - 1)),
                pltpu.SemaphoreType.DMA((2, n - 1)),
                pltpu.SemaphoreType.DMA((2, n - 1)),
            ],
            compiler_params=pltpu.CompilerParams(
                collective_id=0, has_side_effects=True, vmem_limit_bytes=46 * 2 ** 20
            ),
        )(
            weight_gate, moment_gate, square_gate, weight_up, moment_up, square_up,
            norm_gain.reshape(rows // LANES, LANES),
        )
        near = (ready_gate, ready_up, factor_gate.reshape(columns), factor_up.reshape(columns))
        return pl.pallas_call(
            write_out,
            out_shape=tuple(jax.ShapeDtypeStruct(part.shape, part.dtype) for part in near),
            in_specs=[vmem] * 4,
            out_specs=(hbm,) * 4,
            scratch_shapes=[pltpu.SemaphoreType.DMA((4,))],
            compiler_params=pltpu.CompilerParams(vmem_limit_bytes=2 ** 20),
        )(*near)

    split = P(("ens", "zero"), "cols")
    return jax.shard_map(
        per_device,
        mesh=mesh,
        in_specs=(split,) * 6 + (P(("ens", "zero")),),
        out_specs=(P("ens", "cols"), P("ens", "cols"), P(("ens", "cols")), P(("ens", "cols"))),
        check_vma=False,
    )
```
